256 devices in a mesh: prow: 16 (over y_hi, z), pcol: 16 (over x, y_lo, core).
Axes of the slice: x: 4, y: 4 (y_hi: 2, y_lo: 2; y = y_hi * 2 + y_lo), z: 8, core: 2. Of those that a mesh axis runs over, the one named last changes fastest.
Arguments:
- a_panel: float32 [98304, 512], P('prow', 'pcol'), may hold values from -6 to 6
- u_rows: float32 [512, 98304], P('pcol', 'prow'), may hold values from -0.25 to 0.25
- u_col: float32 [98304, 2048], P('prow', 'pcol'), may hold values from -0.01953125 to 0.01953125
- c_in: float32 [98304, 2048], P('prow', 'pcol'), may hold values from -6 to 6
Outputs:
- c_out: float32 [98304, 2048], P('prow', 'pcol')
The draws below stay inside these ranges and needn't reach their ends.
All inputs are finite; a program needn't handle non-finite values.
Results may differ from the reference program's by a relative error of at most 0.00007.
Values sent between devices are 32-bit elements; how exact they have to be, the bound alone decides.
No kernel may reach another device: no remote copies, remote signals or barrier semaphores. Data moves between devices by JAX's collectives and lax.ppermute only.
A program may use at most 128 MiB of HBM per device.

```python
import jax
import jax.numpy as jnp
from jax import lax

N = 98304
SLAB = 2048
KW = 512


def block_scale(own_key, dims, cuts, least, largest):
    level = 1.0
    for axis_at, shards_of in cuts:
        heights = jax.random.uniform(jax.random.fold_in(jax.random.fold_in(own_key, 6), axis_at), (shards_of,), jnp.float32, least / len(cuts), largest / len(cuts))
        level = level * jnp.repeat(jnp.exp(heights), dims[axis_at] // shards_of).reshape((-1,) + (1,) * (len(dims) - 1 - axis_at))
    return level


def scatter_about(stream_key, dims, deviation, bound, split=(), held_as=jnp.bfloat16):
    gain = block_scale(stream_key, dims, split, -0.22, 0.18) if split else 1.0
    entries = jax.random.normal(stream_key, dims, jnp.float32) * deviation * gain
    return jnp.minimum(jnp.maximum(entries, -bound), bound).astype(held_as)


def setup_inputs(seed: int = 0) -> dict:
    arg_keys = jax.random.split(jax.random.key(seed), 5)
    a_panel = scatter_about(arg_keys[0], (N, KW), 1.0, 6.0, ((0, 16), (1, 16)), jnp.float32)
    u_rows = scatter_about(arg_keys[1], (KW, N), KW ** -0.5, 0.25, ((0, 16), (1, 16)), jnp.float32)
    u_col = scatter_about(arg_keys[2], (N, SLAB), N ** -0.5, 0.01953125, ((0, 16), (1, 16)), jnp.float32)
    c_in = scatter_about(arg_keys[3], (N, SLAB), 1.0, 6.0, ((0, 16), (1, 16)), jnp.float32)
    return dict(a_panel=a_panel, u_rows=u_rows, u_col=u_col, c_in=c_in)


def reference(a_panel, u_rows, u_col, c_in):
    inner = jnp.dot(a_panel.T, u_col, precision=lax.Precision.HIGHEST, preferred_element_type=jnp.float32)
    update = jnp.dot(u_rows.T, inner, precision=lax.Precision.HIGHEST, preferred_element_type=jnp.float32)
    return c_in + update
```

```python
import jax
import jax.numpy as jnp
from jax import lax
from jax.sharding import PartitionSpec as P

ROUTES = (
    (0, "+", "+"),
    (0, "y", "-"),
    (0, "-", "y"),
    (2, "+", "y"),
    (2, "-", "-"),
    (1, "+", "y"),
    (5, "-", "y"),
)
C_CHUNKS = 2


def target(at, move):
    x, y, core = at // 4, at // 2 % 2, at % 2
    if move == "y":
        y = 1 - y
    else:
        x = (x + (1 if move == "+" else -1)) % 4
    return (x * 2 + y) * 2 + core


def pairs(moves):
    return [(at, target(at, moves[at % 2])) for at in range(16)]


def gather_blocks(own):
    held = [own]
    for source, *moves in ROUTES:
        held.append(lax.ppermute(held[source], "pcol", pairs(moves)))
    return held


def placed_blocks(blocks):
    k, n = blocks[0].shape
    out = jnp.zeros((k * len(blocks), n), blocks[0].dtype)
    for i, block in enumerate(blocks):
        out = lax.dynamic_update_slice(out, block, (i * k, 0))
    return out


def swapped(x):
    return lax.ppermute(x, "pcol", [(at, at ^ 1) for at in range(16)])


def product(a, b):
    return jnp.dot(a, b, precision=lax.Precision.HIGH, preferred_element_type=jnp.float32)


def on_device(a_panel, u_rows, u_col, c_in):
    other_col = swapped(u_col)
    a = jnp.concatenate(gather_blocks(a_panel.T), axis=0)
    u = gather_blocks(u_rows)
    partial = product(a, jnp.concatenate([u_col, other_col], axis=1))
    tiles = partial.reshape(16, partial.shape[0] // 16, partial.shape[1])
    tiles = lax.all_to_all(tiles, "prow", 0, 0, tiled=True)
    share = jnp.sum(tiles, axis=0)
    copies = jnp.broadcast_to(share, tiles.shape)
    inner = lax.all_to_all(copies, "prow", 0, 0, tiled=True).reshape(partial.shape)
    u = placed_blocks(u)
    rows, width = c_in.shape[0] // C_CHUNKS, c_in.shape[1]
    done = []
    for i in range(C_CHUNKS):
        c = product(u[:, i * rows : (i + 1) * rows].T, inner)
        other = swapped(c[:, width:])
        done.append(c_in[i * rows : (i + 1) * rows] + c[:, :width] + other)
    return jnp.concatenate(done, axis=0)


def solution(mesh):
    placed = (P("prow", "pcol"), P("pcol", "prow"), P("prow", "pcol"), P("prow", "pcol"))
    return jax.shard_map(
        on_device, mesh=mesh, in_specs=placed, out_specs=P("prow", "pcol"), check_vma=False
    )
```

```python
import jax
import jax.numpy as jnp
from jax import lax
from jax.sharding import PartitionSpec as P

ROUTES = (
    (0, "+", "-"),
    (0, "-", "+"),
    (0, "y", "y"),
    (1, "+", "-"),
    (2, "y", "y"),
    (3, "+", "-"),
    (6, "+", "-"),
)
C_CHUNKS = 3


def target(at, move):
    x, y, core = at // 4, at // 2 % 2, at % 2
    if move == "y":
        y = 1 - y
    else:
        x = (x + (1 if move == "+" else -1)) % 4
    return (x * 2 + y) * 2 + core


def pairs(moves):
    return [(at, target(at, moves[at % 2])) for at in range(16)]


def gather_blocks(own):
    held = [own]
    for source, *moves in ROUTES:
        held.append(lax.ppermute(held[source], "pcol", pairs(moves)))
    return held


def placed_blocks(blocks):
    k, n = blocks[0].shape
    out = jnp.zeros((k * len(blocks), n), blocks[0].dtype)
    for i, block in enumerate(blocks):
        out = lax.dynamic_update_slice(out, block, (i * k, 0))
    return out


def swapped(x):
    return lax.ppermute(x, "pcol", [(at, at ^ 1) for at in range(16)])


def product(a, b):
    return jnp.dot(a, b, precision=lax.Precision.HIGH, preferred_element_type=jnp.float32)


def on_device(a_panel, u_rows, u_col, c_in):
    other_col = swapped(u_col)
    a = gather_blocks(a_panel.T)
    u = gather_blocks(u_rows)
    u_cols = jnp.concatenate([u_col, other_col], axis=1)
    shares = []
    for half in range(2):
        part = product(jnp.concatenate(a[half * 4 : half * 4 + 4], axis=0), u_cols)
        tiles = part.reshape(16, part.shape[0] // 16, part.shape[1])
        tiles = lax.all_to_all(tiles, "prow", 0, 0, tiled=True)
        shares.append(jnp.sum(tiles, axis=0))
    copies = jnp.broadcast_to(jnp.stack(shares), (16, 2, *shares[0].shape))
    inner = lax.all_to_all(copies, "prow", 0, 0, tiled=True)
    inner = jnp.moveaxis(inner, 1, 0).reshape(-1, inner.shape[-1])
    u = placed_blocks(u)
    rows, width = c_in.shape[0] // C_CHUNKS, c_in.shape[1]
    done = []
    for i in range(C_CHUNKS):
        c = product(u[:, i * rows : (i + 1) * rows].T, inner)
        other = swapped(c[:, width:])
        done.append(c_in[i * rows : (i + 1) * rows] + c[:, :width] + other)
    return jnp.concatenate(done, axis=0)


def solution(mesh):
    placed = (P("prow", "pcol"), P("pcol", "prow"), P("prow", "pcol"), P("prow", "pcol"))
    return jax.shard_map(
        on_device, mesh=mesh, in_specs=placed, out_specs=P("prow", "pcol"), check_vma=False
    )
```

```python
import jax
import jax.numpy as jnp
from jax import lax
from jax.sharding import PartitionSpec as P

ROUTES = (
    (0, "-", "+"),
    (0, "+", "-"),
    (0, "y", "y"),
    (1, "-", "+"),
    (2, "y", "y"),
    (3, "-", "+"),
    (6, "-", "+"),
)
C_CHUNKS = 3


def target(at, move):
    x, y, core = at // 4, at // 2 % 2, at % 2
    if move == "y":
        y = 1 - y
    else:
        x = (x + (1 if move == "+" else -1)) % 4
    return (x * 2 + y) * 2 + core


def pairs(moves):
    return [(at, target(at, moves[at % 2])) for at in range(16)]


def gather_blocks(own):
    held = [own]
    for source, *moves in ROUTES:
        held.append(lax.ppermute(held[source], "pcol", pairs(moves)))
    return held


def placed_blocks(blocks):
    k, n = blocks[0].shape
    out = jnp.zeros((k * len(blocks), n), blocks[0].dtype)
    for i, block in enumerate(blocks):
        out = lax.dynamic_update_slice(out, block, (i * k, 0))
    return out


def swapped(x):
    return lax.ppermute(x, "pcol", [(at, at ^ 1) for at in range(16)])


def product(a, b):
    return jnp.dot(a, b, precision=lax.Precision.HIGH, preferred_element_type=jnp.float32)


def on_device(a_panel, u_rows, u_col, c_in):
    other_col = swapped(u_col)
    a = gather_blocks(a_panel.T)
    u = gather_blocks(u_rows)
    u_cols = jnp.concatenate([u_col, other_col], axis=1)
    shares = []
    for half in range(2):
        part = product(jnp.concatenate(a[half * 4 : half * 4 + 4], axis=0), u_cols)
        tiles = part.reshape(16, part.shape[0] // 16, part.shape[1])
        tiles = lax.all_to_all(tiles, "prow", 0, 0, tiled=True)
        shares.append(jnp.sum(tiles, axis=0))
    copies = jnp.broadcast_to(jnp.stack(shares), (16, 2, *shares[0].shape))
    inner = lax.all_to_all(copies, "prow", 0, 0, tiled=True)
    inner = jnp.moveaxis(inner, 1, 0).reshape(-1, inner.shape[-1])
    u = placed_blocks(u)
    rows, width = c_in.shape[0] // C_CHUNKS, c_in.shape[1]
    done = []
    for i in range(C_CHUNKS):
        c = product(u[:, i * rows : (i + 1) * rows].T, inner)
        other = swapped(c[:, width:])
        done.append(c_in[i * rows : (i + 1) * rows] + c[:, :width] + other)
    return jnp.concatenate(done, axis=0)


def solution(mesh):
    placed = (P("prow", "pcol"), P("pcol", "prow"), P("prow", "pcol"), P("prow", "pcol"))
    return jax.shard_map(
        on_device, mesh=mesh, in_specs=placed, out_specs=P("prow", "pcol"), check_vma=False
    )
```
